512 devices in a mesh: groups: 2 (over y), fsdp: 32 (over z), tensor: 8 (over x, core).
Axes of the slice: x: 4, y: 2, z: 32, core: 2. Of those that a mesh axis runs over, the one named last changes fastest.
The devices are a block of a 4x8x32 slice.
Arguments:
- tokens: bfloat16 [16384, 4608], P(('groups', 'fsdp'), 'tensor'), parts along dimension 0, may hold values from -100 to 100
- norm_gain: bfloat16 [4608], P('tensor'), may hold values from 0.25 to 1.75
- w_query: bfloat16 [4608, 4096], P('fsdp', 'tensor'), may hold values from -0.5 to 0.5
- w_key: bfloat16 [4608, 2048], P('fsdp', 'tensor'), may hold values from -0.09375 to 0.09375
- w_value: bfloat16 [4608, 2048], P('fsdp', 'tensor'), may hold values from -0.09375 to 0.09375
- w_out: bfloat16 [4096, 4608], P('tensor', 'fsdp'), may hold values from -0.5 to 0.5
- post_gain: bfloat16 [4608], P('tensor'), may hold values from 0.25 to 1.75
Outputs:
- mixed: float32 [16384, 4608], P(('groups', 'fsdp'), 'tensor'), parts along dimension 0
The draws below stay inside these ranges and needn't reach their ends.
There are 2 independent parts, one for each index of `groups`. The reference program is written for one: setup_inputs(seed, part) draws one part's arguments, and reference() takes and returns one part's arrays. A program takes and returns all parts, laid end to end along the dimension named above; an argument that names none is the same for every part. Nothing has to cross between parts.
All inputs are finite; a program needn't handle non-finite values.
Results may differ from the reference program's by a relative error of at most 0.0053.
Values may be sent and summed in bfloat16 or wider, within the bound.
A program may use at most 128 MiB of HBM per device.

```python
import jax
import jax.numpy as jnp
from jax import lax

D = 4608
HEAD_DIM = 128
HEADS = 32
KV_HEADS = 16
LEN = 256
TOKENS = 8192
BLOCK_COLS = 512
N_TENSOR = 8


def draw_tokens(key, part):
    base_key, col_key, row_key = jax.random.split(key, 3)
    col = jnp.arange(D, dtype=jnp.float32) / D
    col_scale = 10.0 ** (col - 0.5 + 0.3 * jax.random.uniform(col_key, (D,), jnp.float32, -1.0, 1.0))
    row_scale = 10.0 ** jax.random.uniform(row_key, (TOKENS, 1), jnp.float32, -0.5, 0.5)
    base = jnp.clip(jax.random.normal(base_key, (TOKENS, D), jnp.float32), -5.0, 5.0)
    return (base * row_scale * col_scale[None, :]).astype(jnp.bfloat16)


def draw_w_out(key, part):
    base_key, col_key = jax.random.split(key, 2)
    rows = HEADS * HEAD_DIM
    col = jnp.arange(D, dtype=jnp.float32) / D
    col_scale = 10.0 ** (0.8 * col - 0.4 + 0.2 * jax.random.uniform(col_key, (D,), jnp.float32, -1.0, 1.0))
    base = jnp.clip(jax.random.normal(base_key, (rows, D), jnp.float32), -5.0, 5.0)
    return (base * col_scale[None, :] / jnp.sqrt(jnp.float32(rows))).astype(jnp.bfloat16)


def shard_levels(stream_key, dims, cuts, least, largest):
    def one(dim, blocks):
        heights = jax.random.uniform(jax.random.fold_in(jax.random.fold_in(stream_key, 6), dim), (blocks,), jnp.float32, least / len(cuts), largest / len(cuts))
        return jnp.repeat(jnp.exp(heights), dims[dim] // blocks).reshape((-1,) + (1,) * (len(dims) - dim - 1))

    factor_of = one(*cuts[0])
    for cut in cuts[1:]:
        factor_of = factor_of * one(*cut)
    return factor_of


def normal_values(rng, extent, spread, limit, shards=(), kind=jnp.bfloat16):
    level = shard_levels(rng, extent, shards, -0.22, 0.18) if shards else 1.0
    array = jax.random.normal(rng, extent, jnp.float32) * spread * level
    return jnp.minimum(jnp.maximum(array, -limit), limit).astype(kind)


def setup_inputs(seed: int = 0, part: int = 0) -> dict:
    streams_of = jax.random.split(jax.random.key(seed), 8)
    part_splits = jax.random.split(jax.random.fold_in(streams_of[7], part), 8)
    tokens = draw_tokens(jax.random.fold_in(jax.random.fold_in(streams_of[7], part), 71), part)
    norm_gain = jnp.clip(1.0 + 0.15 * jax.random.normal(streams_of[1], (D,), jnp.float32), 0.25, 1.75).astype(jnp.bfloat16)
    w_query = normal_values(streams_of[2], (D, HEADS * HEAD_DIM), (D // 36) ** -0.5, 0.5, ((0, 32), (1, 8)))
    w_key = normal_values(streams_of[3], (D, KV_HEADS * HEAD_DIM), D ** -0.5, 0.09375, ((0, 32), (1, 8)))
    w_value = normal_values(streams_of[4], (D, KV_HEADS * HEAD_DIM), D ** -0.5, 0.09375, ((0, 32), (1, 8)))
    w_out = draw_w_out(jax.random.fold_in(streams_of[7], 71), part)
    post_gain = jnp.clip(1.0 + 0.15 * jax.random.normal(streams_of[6], (D,), jnp.float32), 0.25, 1.75).astype(jnp.bfloat16)
    return {"tokens": tokens, "norm_gain": norm_gain, "w_query": w_query, "w_key": w_key, "w_value": w_value, "w_out": w_out, "post_gain": post_gain}


eps_norm = 1e-06
soft_cap = 50.0
attn_scale = 144.0 ** (-0.5)
rope_base = 10000.0

def rotate(values, position):
    head_dim = values.shape[-1]
    half = head_dim // 2
    freq = rope_base ** (-(jnp.arange(half, dtype=jnp.float32) * 2.0 / head_dim))
    angle = position.astype(jnp.float32)[:, None] * freq[None, :]
    cosine = jnp.cos(angle)[:, None, :]
    sine = jnp.sin(angle)[:, None, :]
    first = values[..., :half]
    second = values[..., half:]
    return jnp.concatenate([first * cosine - second * sine, second * cosine + first * sine], axis=-1)

def attend(query, keys, values):
    count, heads, head_dim = query.shape
    kv_count = keys.shape[1]
    grouped = query.reshape(count, kv_count, heads // kv_count, head_dim).astype(jnp.float32)
    scores = jnp.einsum('nkgd,mkd->kgnm', grouped, keys.astype(jnp.float32)) * attn_scale
    capped = soft_cap * jnp.tanh(scores / soft_cap)
    spots = jnp.arange(count)
    allowed = spots[None, :] <= spots[:, None]
    weights = jnp.where(allowed, jnp.exp(capped), 0.0)
    probs = (weights / lax.optimization_barrier(jnp.sum(weights, axis=-1, keepdims=True))).astype(jnp.bfloat16)
    mixed = jnp.einsum('kgnm,mkd->nkgd', probs.astype(jnp.float32), values.astype(jnp.float32))
    return mixed.reshape(count, heads * head_dim).astype(jnp.bfloat16)

def reference(tokens, norm_gain, w_query, w_key, w_value, w_out, post_gain):
    local = tokens.astype(jnp.float32)
    total = lax.optimization_barrier(jnp.sum(local * local, axis=1))
    normed = (local * lax.rsqrt(total / D + eps_norm)[:, None] * norm_gain.astype(jnp.float32)).astype(jnp.bfloat16)
    query_raw = jnp.dot(normed, w_query, preferred_element_type=jnp.float32)
    key_raw = jnp.dot(normed, w_key, preferred_element_type=jnp.float32)
    value_raw = jnp.dot(normed, w_value, preferred_element_type=jnp.float32)
    position = (jnp.arange(TOKENS) % LEN).astype(jnp.int32)
    query = rotate(query_raw.reshape(TOKENS, HEADS, HEAD_DIM), position).astype(jnp.bfloat16)
    key = rotate(key_raw.reshape(TOKENS, KV_HEADS, HEAD_DIM), position).astype(jnp.bfloat16)
    value = value_raw.astype(jnp.bfloat16).reshape(TOKENS, KV_HEADS, HEAD_DIM)
    seq_count = TOKENS // LEN
    attn = lax.map(lambda item: attend(item[0], item[1], item[2]), (query.reshape(seq_count, LEN, HEADS, HEAD_DIM), key.reshape(seq_count, LEN, KV_HEADS, HEAD_DIM), value.reshape(seq_count, LEN, KV_HEADS, HEAD_DIM)))
    attn = attn.reshape(TOKENS, HEADS * HEAD_DIM)
    block = BLOCK_COLS
    proj = jnp.zeros((TOKENS, D), jnp.float32)
    for group in range(N_TENSOR):
        partial_value = jnp.dot(attn[:, group * block:(group + 1) * block], w_out[group * block:(group + 1) * block], preferred_element_type=jnp.float32)
        rounded = lax.optimization_barrier(partial_value.astype(jnp.bfloat16))
        proj = proj + rounded.astype(jnp.float32)
    post_total = lax.optimization_barrier(jnp.sum(proj * proj, axis=1))
    branch = proj * lax.rsqrt(post_total / D + eps_norm)[:, None] * post_gain.astype(jnp.float32)
    return local + branch
```

```python
import functools

import jax
import jax.numpy as jnp
import numpy as np
from jax import lax
from jax.experimental import pallas as pl
from jax.experimental.pallas import tpu as pltpu
from jax.sharding import PartitionSpec as P

HEAD_DIM = 128
EPS = 1e-06
SOFT_CAP = 50.0
ATTN_SCALE = 144.0 ** (-0.5)
ROPE_BASE = 10000.0
MESH = pl.DeviceIdType.MESH
F32 = jnp.float32
BF16 = jnp.bfloat16

PIECES = 3
EARLY = 5
LAG_B, LAG_C, LAG_D = 6, 10, 14


def nt_dot(a, b):
    return lax.dot_general(a, b, (((1,), (1,)), ((), ())), preferred_element_type=F32)


def kernel(
    nz,
    nt,
    tokens_ref,
    gain_ref,
    wq_ref,
    wk_ref,
    wv_ref,
    wo_ref,
    cos_ref,
    sin_ref,
    proj_ref,
    scale_ref,
    tok,
    gain,
    wo_raw,
    cosine,
    sine,
    wqs,
    wos,
    stage,
    nb,
    acc,
    attn,
    pd,
    ybuf,
    sbuf,
    hbuf,
    xbuf,
    fin,
    nat,
    rout,
    tot,
    tot2,
    lsem,
    zqs,
    zqr,
    zws,
    zwr,
    dqs,
    dqr,
    dws,
    dwr,
    tsend,
    trecv,
    usend,
    urecv,
    n1s,
    n1r,
    n2s,
    n2r,
    psend,
    yrecv,
    drecv,
    hsend,
    hrecv,
    xsend,
    xrecv,
):
    g = lax.axis_index("groups")
    z = lax.axis_index("fsdp")
    t = lax.axis_index("tensor")
    y = lax.rem(g, 2)
    g0 = g - y
    x = t // 2
    c = lax.rem(t, 2)
    nx = nt // 2
    per_t = nz // nt
    half = nz // 2
    rows, width = tok.shape
    d_model = width * nt
    chunk = wqs.shape[2]
    piece = chunk // PIECES
    zn = (lax.rem(z + 1, nz), lax.rem(z + nz - 1, nz))
    xp, xm = lax.rem(x + 1, nx), lax.rem(x + nx - 1, nx)
    peer = (g, z, 2 * x + 1 - c)
    q_last = (half, half - 1)
    w_last = (half - 1, half)

    def local(src, dst, i):
        return pltpu.make_async_copy(src, dst, lsem.at[i])

    def remote(src, dst, ss, rs, dev):
        return pltpu.make_async_remote_copy(
            src_ref=src, dst_ref=dst, send_sem=ss, recv_sem=rs, device_id=dev, device_id_type=MESH
        )

    yq = pl.multiple_of(y * 256, 128)
    yk = pl.multiple_of(y * 128, 128)
    loads = [
        local(wq_ref.at[:, pl.ds(yq, 256)], wqs.at[c, z, :, pl.ds(0, 256)], 0),
        local(wk_ref.at[:, pl.ds(yk, 128)], wqs.at[c, z, :, pl.ds(256, 128)], 1),
        local(wv_ref.at[:, pl.ds(yk, 128)], wqs.at[c, z, :, pl.ds(384, 128)], 2),
        local(tokens_ref, tok, 3),
        local(gain_ref, gain, 4),
        local(wo_ref.at[pl.ds(yq, 256)], wo_raw, 5),
        local(cos_ref, cosine, 6),
        local(sin_ref, sine, 7),
    ]
    for load in loads:
        load.start()

    barrier = pltpu.get_barrier_semaphore()
    partners = [(g, zn[0], t), (g, zn[1], t)]
    partners += [(g, z, lax.rem(t + i, nt)) for i in range(1, nt)]
    partners += [(g0 + 1 - y, z, 2 * x), (g0 + 1 - y, z, 2 * x + 1)]
    for dev in partners:
        pl.semaphore_signal(barrier, inc=1, device_id=dev, device_id_type=MESH)
    pl.semaphore_wait(barrier, len(partners))

    def source(d, k):
        return lax.rem(z - k + nz, nz) if d == 0 else lax.rem(z + k, nz)

    def order(d, k, last):
        if isinstance(k, int) and k == 0:
            return 0
        return 2 * k - 1 if d == 0 or (isinstance(k, int) and k == half) else 2 * k

    def ring_copy(buf, ss, rs, d, k, sem_k, p):
        ref = buf.at[c, source(d, k), pl.ds(p * piece, piece)]
        return remote(ref, ref, ss.at[d, sem_k, p], rs.at[d, sem_k, p], (g, zn[d], t))

    def across(buf, ss, rs, s, i):
        ref = buf.at[c, s]
        return remote(ref, ref, ss.at[i], rs.at[i], peer)

    def across_in(buf, ss, rs, s, i):
        ref = buf.at[1 - c, s]
        return remote(ref, ref, ss.at[i], rs.at[i], peer)

    q_ring = (wqs, zqs, zqr, dqs, dqr, q_last)
    w_ring = (wos, zws, zwr, dws, dwr, w_last)

    def ring_start(ring):
        buf, ss, rs, ds, dr, last = ring
        for p in range(PIECES):
            for d in range(2):
                ring_copy(buf, ss, rs, d, 0, 0, p).start()
        across(buf, ds, dr, z, 0).start()

    def ring_step(ring, k):
        buf, ss, rs, ds, dr, last = ring
        dirs = [d for d in range(2) if not isinstance(k, int) or k <= last[d]]
        for p in range(PIECES):
            for d in dirs:
                ring_copy(buf, ss, rs, d, k, k - 1, p).wait_recv()
                if not isinstance(k, int) or k < last[d]:
                    ring_copy(buf, ss, rs, d, k, k, p).start()
        for d in dirs:
            across(buf, ds, dr, source(d, k), order(d, k, last)).start()

    def across_wait(ring, k):
        buf, ss, rs, ds, dr, last = ring
        for d in range(2):
            if not isinstance(k, int) or k <= last[d]:
                across_in(buf, ds, dr, source(d, k), order(d, k, last)).wait_recv()

    for i in (0, 1, 2):
        loads[i].wait()
    ring_start(q_ring)

    def as_row(column):
        return jnp.broadcast_to(column, (rows, 128)).T[0:8]

    def as_column(row):
        return jnp.broadcast_to(row, (128, rows)).T

    def share(buf, ss, rs):
        return [
            remote(buf.at[t], buf.at[t], ss.at[i], rs.at[t], (g, z, lax.rem(t + i, nt)))
            for i in range(1, nt)
        ]

    def share_wait(buf, ss, rs):
        for i in range(1, nt):
            o = lax.rem(t + nt - i, nt)
            remote(buf.at[o], buf.at[o], ss.at[i], rs.at[o], peer).wait_recv()

    def total_scale(buf):
        total = buf[0, 0:1]
        for i in range(1, nt):
            total = total + buf[i, 0:1]
        return as_column(lax.rsqrt(total / d_model + EPS))

    loads[3].wait()
    values = tok[...].astype(F32)
    tot[t] = as_row(jnp.sum(values * values, axis=1, keepdims=True))
    for copy in share(tot, tsend, trecv):
        copy.start()

    loads[4].wait()
    loads[5].wait()
    wos[c, z] = wo_raw[...].astype(F32).T.astype(BF16)

    def first_hop(to_y):
        return remote(stage, nb.at[t], n1s.at[to_y], n1r.at[c], (g0 + to_y, z, 2 * x + y))

    def normalize():
        share_wait(tot, tsend, trecv)
        scale = total_scale(tot)[:, 0:1]
        stage[...] = (tok[...].astype(F32) * scale * gain[...].astype(F32)).astype(BF16)
        first_hop_other = remote(
            stage, nb.at[t], n1s.at[0], n1r.at[c], (g0 + 1 - y, z, 2 * x + y)
        )
        first_hop_other.start()

        @pl.when(c == y)
        def _():
            nb[t] = stage[...]

        @pl.when(c != y)
        def _():
            remote(stage, nb.at[t], n1s.at[1], n1r.at[c], peer).start()

    def round_x(shard, to, i):
        return remote(
            nb.at[shard], nb.at[shard], n2s.at[i], n2r.at[shard], (g, z, 2 * to + c)
        )

    def first_arrivals():
        for i in range(2):
            shard = 2 * x + i

            @pl.when((y != c) | (c != i))
            def _():
                remote(nb.at[shard], nb.at[shard], n1s.at[0], n1r.at[i], peer).wait_recv()

            round_x(shard, xp, 2 * i).start()
            round_x(shard, xm, 2 * i + 1).start()

    def x_wait(shard):
        round_x(shard, xp, 0).wait_recv()

    def relay():
        x_wait(2 * xm)
        round_x(2 * xm, xp, 4).start()
        x_wait(2 * xp + 1)
        round_x(2 * xp + 1, xm, 5).start()

    def last_arrivals():
        opposite = lax.rem(x + 2, nx)
        x_wait(2 * xm + 1)
        x_wait(2 * xp)
        x_wait(2 * opposite)
        x_wait(2 * opposite + 1)

    first_block = z // per_t

    def block(i, init=False):
        o = lax.rem(first_block + i + nt, nt)
        feats = nb[o]
        for u in range(2):
            w = wqs[u, pl.ds(o * per_t, per_t)].reshape(width, wqs.shape[3])
            part = jnp.dot(feats, w, preferred_element_type=F32)
            acc[u] = part if init else acc[u] + part

    def rotary(values):
        return values * cosine[...] + pltpu.roll(values, HEAD_DIM // 2, 1) * sine[...]

    def attend(u):
        key = rotary(acc[u, :, 256:384]).astype(BF16)
        value = acc[u, :, 384:512].astype(BF16)
        spot_q = lax.broadcasted_iota(jnp.int32, (rows, rows), 0)
        spot_k = lax.broadcasted_iota(jnp.int32, (rows, rows), 1)
        for h in range(2):
            query = rotary(acc[u, :, h * 128 : (h + 1) * 128]).astype(BF16)
            scores = nt_dot(query, key) * ATTN_SCALE
            e = jnp.exp(SOFT_CAP * jnp.tanh(scores / SOFT_CAP))
            e = jnp.where(spot_k <= spot_q, e, 0.0)
            probs = (e / jnp.sum(e, axis=1, keepdims=True)).astype(BF16)
            out = jnp.dot(probs, value, preferred_element_type=F32)
            attn[u, :, h * 128 : (h + 1) * 128] = out.astype(BF16)

    def chunk_of(q):
        k = (q + 1) // 2
        s = lax.rem(jnp.where(lax.rem(q, 2) == 1, z - k + nz, z + k), nz)
        o = s // per_t
        return s, o, o // 2, lax.rem(o, 2)

    def to_peer(s, oc):
        return remote(pd.at[0, s], pd.at[1, s], psend.at[s], drecv.at[s], (g, z, 2 * x + oc))

    def to_pair(s, oc):
        return remote(
            pd.at[0, s], ybuf.at[s], psend.at[s], yrecv.at[s], (g0 + 1 - y, z, 2 * x + oc)
        )

    def stage_a(q):
        s, o, ox, oc = chunk_of(q)
        across_in(wos, dws, dwr, s, q).wait_recv()
        part = nt_dot(wos[0, s], attn[0]) + nt_dot(wos[1, s], attn[1])
        pd[0, s] = part.astype(BF16)

        @pl.when((y == c) & (oc != c))
        def _():
            to_peer(s, oc).start()

        @pl.when(y != c)
        def _():
            to_pair(s, oc).start()

    away = jnp.where(y == c, 0, 1)

    def pair_sum(s):
        to_pair(s, c).wait_recv()

        @pl.when(y != c)
        def _():
            to_peer(s, c).wait_recv()

        return pd[away, s].astype(F32) + ybuf[s].astype(F32)

    def to_side(s, i):
        return remote(
            sbuf.at[s, :, pl.ds(128 * i, 128)],
            hbuf.at[s],
            hsend.at[i, s],
            hrecv.at[s],
            (g, z, 2 * (xp, xm)[i] + c),
        )

    def stage_b(q):
        s, o, ox, oc = chunk_of(q)
        dx = lax.rem(x - ox + nx, nx)

        @pl.when((oc == c) & (dx == 2))
        def _():
            sbuf[s] = pair_sum(s).astype(BF16)
            to_side(s, 0).start()
            to_side(s, 1).start()

    def to_owner(s, side, ox):
        return remote(
            sbuf.at[s], xbuf.at[side, s], xsend.at[s], xrecv.at[side, s], (g, z, 2 * ox + c)
        )

    def stage_c(q):
        s, o, ox, oc = chunk_of(q)
        dx = lax.rem(x - ox + nx, nx)

        @pl.when((oc == c) & ((dx == 1) | (dx == 3)))
        def _():
            total = pair_sum(s)
            to_side(s, 0).wait_recv()
            extra = hbuf[s].astype(F32)
            sbuf[s, :, 0:128] = (total[:, 0:128] + jnp.where(dx == 3, extra, 0.0)).astype(BF16)
            sbuf[s, :, 128:256] = (total[:, 128:256] + jnp.where(dx == 1, extra, 0.0)).astype(BF16)
            to_owner(s, dx // 2, ox).start()

    def stage_d(q):
        s, o, ox, oc = chunk_of(q)

        @pl.when(o == t)
        def _():
            total = pair_sum(s)
            for side in range(2):
                to_owner(s, side, x).wait_recv()
                total = total + xbuf[side, s].astype(F32)
            fin[lax.rem(s, per_t)] = total

    stages = ((stage_a, 0), (stage_b, LAG_B), (stage_c, LAG_C), (stage_d, LAG_D))

    def reduce_chunks(low, high):
        for fn, lag in stages:
            lo, hi = low - lag, high - lag
            if isinstance(lo, int):
                lo, hi = max(lo, 0), max(hi, 0)
            else:
                lo, hi = jnp.maximum(lo, 0), jnp.maximum(hi, 0)

            @pl.loop(lo, hi)
            def _(q):
                fn(q)

    w_start = half - EARLY
    block_after = {
        half - 4: [(0, True), (1, False)],
        half - 3: [(-1, False), (2, False)],
        half - 2: [(-2, False)],
    }
    for k in range(1, half + 1):
        ring_step(q_ring, k)
        if k == w_start:
            ring_start(w_ring)
        if k > w_start:
            ring_step(w_ring, k - w_start)
        if k > 1:
            across_wait(q_ring, k - 1)
        if k == 1:
            across_in(wqs, dqs, dqr, z, 0).wait_recv()
            normalize()
        if k == 3:
            first_arrivals()
        if k == 7:
            relay()
        if k == 11:
            last_arrivals()
        for i, init in block_after.get(k, []):
            block(i, init)

    done = EARLY
    block(3)
    block(-3)
    done += 1
    ring_step(w_ring, done)
    across_wait(q_ring, half)
    block(4)
    loads[6].wait()
    loads[7].wait()
    attend(0)
    done += 1
    ring_step(w_ring, done)
    attend(1)
    done += 1
    ring_step(w_ring, done)

    def ready(i):
        if isinstance(i, int):
            return max(min(4 * (i - done), 2 * i - 1), 0)
        return jnp.maximum(jnp.minimum(4 * (i - done), 2 * i - 1), 0)

    @pl.loop(done + 1, half - 1)
    def _(i):
        ring_step(w_ring, i)
        reduce_chunks(ready(i - 1), ready(i))

    for i in (half - 1, half):
        ring_step(w_ring, i)
        reduce_chunks(ready(i - 1), ready(i))
    at = ready(half)

    @pl.loop(at, nz)
    def _(q):
        stage_a(q)

    for fn, lag in stages[1:]:

        @pl.loop(max(at - lag, 0), nz)
        def _(q):
            fn(q)

    whole = fin[...].reshape(width, rows)
    square = jnp.sum(whole * whole, axis=0, keepdims=True)
    tot2[t] = jnp.broadcast_to(square, (8, rows))
    for copy in share(tot2, usend, urecv):
        copy.start()
    nat[...] = whole.T
    out = local(nat, proj_ref, 8)
    out.start()

    for ring in (q_ring, w_ring):
        buf, ss, rs, ds, dr, last = ring
        for d in range(2):

            @pl.loop(0, last[d])
            def _(k):
                for p in range(PIECES):
                    ring_copy(buf, ss, rs, d, k, k, p).wait_send()

        @pl.loop(0, nz)
        def _(i):
            across(buf, ds, dr, z, i).wait_send()

    for copy in share(tot, tsend, trecv):
        copy.wait_send()
    remote(stage, nb.at[t], n1s.at[0], n1r.at[c], (g0 + 1 - y, z, 2 * x + y)).wait_send()

    @pl.when(c != y)
    def _():
        remote(stage, nb.at[t], n1s.at[1], n1r.at[c], peer).wait_send()

    for i in range(6):
        round_x(0, xp, i).wait_send()

    @pl.loop(0, nz)
    def _(q):
        s, o, ox, oc = chunk_of(q)
        dx = lax.rem(x - ox + nx, nx)

        @pl.when((y != c) | (oc != c))
        def _():
            to_peer(s, 1 - c).wait_send()

        @pl.when((oc == c) & (dx == 2))
        def _():
            to_side(s, 0).wait_send()
            to_side(s, 1).wait_send()

        @pl.when((oc == c) & ((dx == 1) | (dx == 3)))
        def _():
            to_owner(s, 0, xp).wait_send()

    share_wait(tot2, usend, urecv)
    rout[...] = total_scale(tot2)
    out2 = local(rout, scale_ref, 9)
    out2.start()
    for copy in share(tot2, usend, urecv):
        copy.wait_send()
    out.wait()
    out2.wait()


def rope_tables(length):
    half = HEAD_DIM // 2
    freq = np.float32(ROPE_BASE) ** (-(np.arange(half, dtype=np.float32) * np.float32(2.0) / np.float32(HEAD_DIM)))
    angle = np.arange(length, dtype=np.float32)[:, None] * freq.astype(np.float32)[None, :]
    cosine, sine = np.cos(angle), np.sin(angle)
    return (
        np.concatenate([cosine, cosine], axis=1).astype(np.float32),
        np.concatenate([-sine, sine], axis=1).astype(np.float32),
    )


def on_device(nz, nt, tokens, norm_gain, w_query, w_key, w_value, w_out, post_gain):
    rows, width = tokens.shape
    depth = w_query.shape[0]
    cosine, sine = rope_tables(rows)
    q_cols = w_query.shape[1] // 2
    qkv = q_cols + w_key.shape[1] // 2 + w_value.shape[1] // 2
    dma = pltpu.SemaphoreType.DMA
    half = nz // 2
    vm = pltpu.VMEM
    hbm = pl.BlockSpec(memory_space=pl.ANY)
    proj, scale = pl.pallas_call(
        functools.partial(kernel, nz, nt),
        out_shape=(
            jax.ShapeDtypeStruct((rows, width), F32),
            jax.ShapeDtypeStruct((rows, 128), F32),
        ),
        in_specs=[hbm] * 8,
        out_specs=(hbm, hbm),
        scratch_shapes=[
            vm((rows, width), BF16),
            vm((1, width), BF16),
            vm((q_cols, depth), BF16),
            vm((rows, HEAD_DIM), F32),
            vm((rows, HEAD_DIM), F32),
            vm((2, nz, depth, qkv), BF16),
            vm((2, nz, depth, q_cols), BF16),
            vm((rows, width), BF16),
            vm((nt, rows, width), BF16),
            vm((2, rows, qkv), F32),
            vm((2, rows, q_cols), BF16),
            vm((2, nz, depth, rows), BF16),
            vm((nz, depth, rows), BF16),
            vm((nz, depth, rows), BF16),
            vm((nz, depth, 128), BF16),
            vm((2, nz, depth, rows), BF16),
            vm((nz // nt, depth, rows), F32),
            vm((rows, width), F32),
            vm((rows, 128), F32),
            vm((nt, 8, rows), F32),
            vm((nt, 8, rows), F32),
            dma((10,)),
            dma((2, half, PIECES)),
            dma((2, half, PIECES)),
            dma((2, half, PIECES)),
            dma((2, half, PIECES)),
            dma((nz,)),
            dma((nz,)),
            dma((nz,)),
            dma((nz,)),
            dma((nt,)),
            dma((nt,)),
            dma((nt,)),
            dma((nt,)),
            dma((2,)),
            dma((2,)),
            dma((6,)),
            dma((nt,)),
            dma((nz,)),
            dma((nz,)),
            dma((nz,)),
            dma((2, nz)),
            dma((nz,)),
            dma((nz,)),
            dma((2, nz)),
        ],
        compiler_params=pltpu.CompilerParams(
            collective_id=0, has_side_effects=True, vmem_limit_bytes=60 * 1024 * 1024
        ),
        name="attention_block",
    )(
        tokens,
        norm_gain.reshape(1, width),
        w_query,
        w_key,
        w_value,
        w_out,
        jnp.asarray(cosine),
        jnp.asarray(sine),
    )
    branch = proj * scale[:, 0:1] * post_gain.astype(F32)
    return tokens.astype(F32) + branch


def solution(mesh):
    nz, nt = mesh.shape["fsdp"], mesh.shape["tensor"]
    placed = (
        P(("groups", "fsdp"), "tensor"),
        P("tensor"),
        P("fsdp", "tensor"),
        P("fsdp", "tensor"),
        P("fsdp", "tensor"),
        P("tensor", "fsdp"),
        P("tensor"),
    )
    return jax.shard_map(
        functools.partial(on_device, nz, nt),
        mesh=mesh,
        in_specs=placed,
        out_specs=P(("groups", "fsdp"), "tensor"),
        check_vma=False,
    )
```

```python
import functools

import jax
import jax.numpy as jnp
import numpy as np
from jax import lax
from jax.experimental import pallas as pl
from jax.experimental.pallas import tpu as pltpu
from jax.sharding import PartitionSpec as P

HEAD_DIM = 128
EPS = 1e-06
SOFT_CAP = 50.0
ATTN_SCALE = 144.0 ** (-0.5)
ROPE_BASE = 10000.0
MESH = pl.DeviceIdType.MESH
F32 = jnp.float32
BF16 = jnp.bfloat16

PIECES = 3
EARLY = 8
SLOTS = 4


def nt_dot(a, b):
    return lax.dot_general(a, b, (((1,), (1,)), ((), ())), preferred_element_type=F32)


def kernel(
    nz,
    nt,
    tokens_ref,
    gain_ref,
    wq_ref,
    wk_ref,
    wv_ref,
    wo_ref,
    post_ref,
    cos_ref,
    sin_ref,
    out_ref,
    tok,
    gain,
    post,
    pgain,
    cosine,
    sine,
    wqs,
    wos,
    stage,
    nb,
    acc,
    attn,
    pd,
    ybuf,
    sbuf,
    hbuf,
    xbuf,
    fin,
    res,
    tot,
    tot2,
    lsem,
    zqs,
    zqr,
    zws,
    zwr,
    dqs,
    dqr,
    dws,
    dwr,
    tsend,
    trecv,
    usend,
    urecv,
    n1s,
    n1r,
    n2s,
    n2r,
    psend,
    yrecv,
    drecv,
    hsend,
    hrecv,
    xsend,
    xrecv,
):
    g = lax.axis_index("groups")
    z = lax.axis_index("fsdp")
    t = lax.axis_index("tensor")
    y = lax.rem(g, 2)
    g0 = g - y
    x = t // 2
    c = lax.rem(t, 2)
    nx = nt // 2
    per_t = nz // nt
    half = nz // 2
    width, rows = tok.shape
    d_model = width * nt
    chunk = wqs.shape[2]
    piece = chunk // PIECES
    zn = (lax.rem(z + 1, nz), lax.rem(z + nz - 1, nz))
    xp, xm = lax.rem(x + 1, nx), lax.rem(x + nx - 1, nx)
    peer = (g, z, 2 * x + 1 - c)
    q_last = (half, half - 1)
    w_last = (half - 1, half)

    def local(src, dst, i):
        return pltpu.make_async_copy(src, dst, lsem.at[i])

    def remote(src, dst, ss, rs, dev):
        return pltpu.make_async_remote_copy(
            src_ref=src, dst_ref=dst, send_sem=ss, recv_sem=rs, device_id=dev, device_id_type=MESH
        )

    yq = pl.multiple_of(y * 256, 128)
    yk = pl.multiple_of(y * 128, 128)
    loads = [
        local(wq_ref.at[:, pl.ds(yq, 256)], wqs.at[c, z, :, pl.ds(0, 256)], 0),
        local(wk_ref.at[:, pl.ds(yk, 128)], wqs.at[c, z, :, pl.ds(256, 128)], 1),
        local(wv_ref.at[:, pl.ds(yk, 128)], wqs.at[c, z, :, pl.ds(384, 128)], 2),
        local(tokens_ref, tok, 3),
        local(gain_ref, gain, 4),
        local(wo_ref.at[:, pl.ds(yq, 256)], wos.at[c, z], 5),
        local(cos_ref, cosine, 6),
        local(sin_ref, sine, 7),
        local(post_ref, post, 8),
    ]
    for load in loads:
        load.start()

    barrier = pltpu.get_barrier_semaphore()
    partners = [(g, zn[0], t), (g, zn[1], t)]
    partners += [(g, z, lax.rem(t + i, nt)) for i in range(1, nt)]
    partners += [(g0 + 1 - y, z, 2 * x), (g0 + 1 - y, z, 2 * x + 1)]
    for dev in partners:
        pl.semaphore_signal(barrier, inc=1, device_id=dev, device_id_type=MESH)
    pl.semaphore_wait(barrier, len(partners))

    def source(d, k):
        return lax.rem(z - k + nz, nz) if d == 0 else lax.rem(z + k, nz)

    def order(d, k, last):
        if isinstance(k, int) and k == 0:
            return 0
        return 2 * k - 1 if d == 0 or (isinstance(k, int) and k == half) else 2 * k

    def ring_copy(buf, ss, rs, d, k, sem_k, p):
        ref = buf.at[c, source(d, k), pl.ds(p * piece, piece)]
        return remote(ref, ref, ss.at[d, 0, p], rs.at[d, sem_k, p], (g, zn[d], t))

    def across_in(buf, ss, rs, s, i):
        ref = buf.at[1 - c, s]
        return remote(ref, ref, ss.at[0, 0], rs.at[i], peer)

    q_ring = (wqs, zqs, zqr, dqs, dqr, q_last)
    w_ring = (wos, zws, zwr, dws, dwr, w_last)

    def slot(k):
        return k % SLOTS if isinstance(k, int) else lax.rem(k, SLOTS)

    def ring_send(ring, d, k, p):
        buf, ss, rs, ds, dr, last = ring
        ref = buf.at[c, source(d, k), pl.ds(p * piece, piece)]
        return remote(ref, ref, ss.at[d, slot(k), p], rs.at[d, k, p], (g, zn[d], t))

    def across_send(ring, d, k):
        buf, ss, rs, ds, dr, last = ring
        ref = buf.at[c, source(d, k)]
        return remote(ref, ref, ds.at[d, slot(k)], dr.at[order(d, k, last)], peer)

    def guarded(k, fn):
        if isinstance(k, int):
            if k >= SLOTS:
                fn()
        else:
            pl.when(k >= SLOTS)(fn)

    def ring_start(ring):
        for p in range(PIECES):
            for d in range(2):
                ring_send(ring, d, 0, p).start()
        across_send(ring, 0, 0).start()

    def ring_step(ring, k):
        buf, ss, rs, ds, dr, last = ring
        dirs = [d for d in range(2) if not isinstance(k, int) or k <= last[d]]
        for p in range(PIECES):
            for d in dirs:
                ring_copy(buf, ss, rs, d, k, k - 1, p).wait_recv()
                if not isinstance(k, int) or k < last[d]:
                    guarded(k, lambda: ring_send(ring, d, k, p).wait_send())
                    ring_send(ring, d, k, p).start()
        for d in dirs:
            if d == 0:
                guarded(k, lambda: across_send(ring, d, k).wait_send())
            elif isinstance(k, int):
                if k > SLOTS:
                    across_send(ring, d, k).wait_send()
            else:
                pl.when(k > SLOTS)(lambda: across_send(ring, d, k).wait_send())
            across_send(ring, d, k).start()

    def ring_drain(ring):
        buf, ss, rs, ds, dr, last = ring
        for d in range(2):
            for k in range(last[d] - SLOTS, last[d]):
                for p in range(PIECES):
                    ring_send(ring, d, k, p).wait_send()
            for k in range(last[d] - SLOTS + 1, last[d] + 1):
                across_send(ring, d, k).wait_send()

    def across_wait(ring, k):
        buf, ss, rs, ds, dr, last = ring
        for d in range(2):
            if not isinstance(k, int) or k <= last[d]:
                across_in(buf, ds, dr, source(d, k), order(d, k, last)).wait_recv()

    for i in (0, 1, 2):
        loads[i].wait()
    ring_start(q_ring)

    def share(buf, ss, rs):
        return [
            remote(buf.at[t], buf.at[t], ss.at[i], rs.at[t], (g, z, lax.rem(t + i, nt)))
            for i in range(1, nt)
        ]

    def share_wait(buf, ss, rs):
        for i in range(1, nt):
            o = lax.rem(t + nt - i, nt)
            remote(buf.at[o], buf.at[o], ss.at[i], rs.at[o], peer).wait_recv()

    def total_scale(buf):
        total = buf[0, 0:1]
        for i in range(1, nt):
            total = total + buf[i, 0:1]
        return lax.rsqrt(total / d_model + EPS)

    loads[3].wait()
    values = tok[...].astype(F32)
    tot[t] = jnp.broadcast_to(jnp.sum(values * values, axis=0, keepdims=True), (8, rows))
    for copy in share(tot, tsend, trecv):
        copy.start()

    loads[4].wait()
    loads[5].wait()
    loads[8].wait()
    pgain[...] = jnp.broadcast_to(post[...].astype(F32).reshape(1, width), (128, width)).T

    def first_hop(to_y):
        return remote(stage, nb.at[t], n1s.at[to_y], n1r.at[c], (g0 + to_y, z, 2 * x + y))

    def normalize():
        share_wait(tot, tsend, trecv)
        scaled = (tok[...].astype(F32) * total_scale(tot)).T
        stage[...] = (scaled * gain[...].astype(F32).reshape(1, width)).astype(BF16)
        first_hop_other = remote(
            stage, nb.at[t], n1s.at[0], n1r.at[c], (g0 + 1 - y, z, 2 * x + y)
        )
        first_hop_other.start()

        @pl.when(c == y)
        def _():
            nb[t] = stage[...]

        @pl.when(c != y)
        def _():
            remote(stage, nb.at[t], n1s.at[1], n1r.at[c], peer).start()

    def round_x(shard, to, i):
        return remote(
            nb.at[shard], nb.at[shard], n2s.at[i], n2r.at[shard], (g, z, 2 * to + c)
        )

    def first_arrivals():
        for i in range(2):
            shard = 2 * x + i

            @pl.when((y != c) | (c != i))
            def _():
                remote(nb.at[shard], nb.at[shard], n1s.at[0], n1r.at[i], peer).wait_recv()

            round_x(shard, xp, 2 * i).start()
            round_x(shard, xm, 2 * i + 1).start()

    def x_wait(shard):
        round_x(shard, xp, 0).wait_recv()

    def relay():
        x_wait(2 * xm)
        round_x(2 * xm, xp, 4).start()
        x_wait(2 * xp + 1)
        round_x(2 * xp + 1, xm, 5).start()

    def last_arrivals():
        opposite = lax.rem(x + 2, nx)
        x_wait(2 * xm + 1)
        x_wait(2 * xp)
        x_wait(2 * opposite)
        x_wait(2 * opposite + 1)

    first_block = z // per_t

    def block(i, init=False):
        o = lax.rem(first_block + i + nt, nt)
        feats = nb[o]
        for u in range(2):
            w = wqs[u, pl.ds(o * per_t, per_t)].reshape(width, wqs.shape[3])
            part = jnp.dot(feats, w, preferred_element_type=F32)
            acc[u] = part if init else acc[u] + part

    def rotary(values):
        return values * cosine[...] + pltpu.roll(values, HEAD_DIM // 2, 1) * sine[...]

    def attend(u):
        key = rotary(acc[u, :, 256:384]).astype(BF16)
        value = acc[u, :, 384:512].astype(BF16)
        spot_q = lax.broadcasted_iota(jnp.int32, (rows, rows), 0)
        spot_k = lax.broadcasted_iota(jnp.int32, (rows, rows), 1)
        for h in range(2):
            query = rotary(acc[u, :, h * 128 : (h + 1) * 128]).astype(BF16)
            scores = nt_dot(query, key) * ATTN_SCALE
            e = jnp.exp(SOFT_CAP * jnp.tanh(scores / SOFT_CAP))
            e = jnp.where(spot_k <= spot_q, e, 0.0)
            probs = (e / jnp.sum(e, axis=1, keepdims=True)).astype(BF16)
            out = jnp.dot(probs, value, preferred_element_type=F32)
            attn[u, :, h * 128 : (h + 1) * 128] = out.astype(BF16)

    def chunk_of(q):
        k = (q + 1) // 2
        s = lax.rem(jnp.where(lax.rem(q, 2) == 1, z - k + nz, z + k), nz)
        o = s // per_t
        return s, o, o // 2, lax.rem(o, 2)

    def owned(s):
        return s // (2 * per_t) * per_t + lax.rem(s, per_t)

    def to_peer(s, oc):
        return remote(
            pd.at[0, s], pd.at[1, s], psend.at[s], drecv.at[owned(s)], (g, z, 2 * x + oc)
        )

    def to_pair(s, oc):
        return remote(
            pd.at[0, s],
            ybuf.at[s],
            psend.at[s],
            yrecv.at[owned(s)],
            (g0 + 1 - y, z, 2 * x + oc),
        )

    def stage_a(q):
        s, o, ox, oc = chunk_of(q)
        across_in(wos, dws, dwr, s, q).wait_recv()
        part = nt_dot(wos[0, s], attn[0]) + nt_dot(wos[1, s], attn[1])
        pd[0, s] = part.astype(BF16)

        @pl.when((y == c) & (oc != c))
        def _():
            to_peer(s, oc).start()

        @pl.when(y != c)
        def _():
            to_pair(s, oc).start()

    away = jnp.where(y == c, 0, 1)

    def pair_sum(s):
        to_pair(s, c).wait_recv()

        @pl.when(y != c)
        def _():
            to_peer(s, c).wait_recv()

        return pd[away, s].astype(F32) + ybuf[s].astype(F32)

    def to_side(s, i):
        return remote(
            sbuf.at[s, :, pl.ds(128 * i, 128)],
            hbuf.at[s],
            hsend.at[i, lax.rem(s, per_t)],
            hrecv.at[i, lax.rem(s, per_t)],
            (g, z, 2 * (xp, xm)[i] + c),
        )

    def stage_b(q):
        s, o, ox, oc = chunk_of(q)
        dx = lax.rem(x - ox + nx, nx)

        @pl.when((oc == c) & (dx == 2))
        def _():
            sbuf[s] = pair_sum(s).astype(BF16)
            to_side(s, 0).start()
            to_side(s, 1).start()

    def to_owner(s, side, ox):
        return remote(
            sbuf.at[s],
            xbuf.at[side, s],
            xsend.at[side, lax.rem(s, per_t)],
            xrecv.at[side, lax.rem(s, per_t)],
            (g, z, 2 * ox + c),
        )

    def stage_c(q):
        s, o, ox, oc = chunk_of(q)
        dx = lax.rem(x - ox + nx, nx)

        @pl.when((oc == c) & ((dx == 1) | (dx == 3)))
        def _():
            total = pair_sum(s)
            @pl.when(dx == 3)
            def _():
                to_side(s, 0).wait_recv()

            @pl.when(dx == 1)
            def _():
                to_side(s, 1).wait_recv()

            extra = hbuf[s].astype(F32)
            sbuf[s, :, 0:128] = (total[:, 0:128] + jnp.where(dx == 3, extra, 0.0)).astype(BF16)
            sbuf[s, :, 128:256] = (total[:, 128:256] + jnp.where(dx == 1, extra, 0.0)).astype(BF16)
            to_owner(s, dx // 2, ox).start()

    def stage_d(q):
        s, o, ox, oc = chunk_of(q)

        @pl.when(o == t)
        def _():
            total = pair_sum(s)
            for side in range(2):
                to_owner(s, side, x).wait_recv()
                total = total + xbuf[side, s].astype(F32)
            fin[lax.rem(s, per_t)] = total

    def clipped(value, low, high):
        if isinstance(value, int):
            return max(min(value, high), low)
        return jnp.maximum(jnp.minimum(value, high), low)

    def reached(i):
        a = clipped(8 * (i - EARLY), 0, 2 * i - 1)
        b = clipped(4 * (i - EARLY) - 8, 0, a)
        return a, b, clipped(b - 4, 0, b), clipped(b - 8, 0, b)

    def reduce_chunks(low, high):
        for fn, lo, hi in zip((stage_a, stage_b, stage_c, stage_d), low, high):

            @pl.loop(lo, hi)
            def _(q):
                fn(q)

    w_start = half - EARLY
    block_after = {
        half - 4: [(0, True), (1, False)],
        half - 3: [(-1, False), (2, False)],
        half - 2: [(-2, False)],
    }
    for k in range(1, half + 1):
        ring_step(q_ring, k)
        if k == w_start:
            ring_start(w_ring)
        if k > w_start:
            ring_step(w_ring, k - w_start)
        if k > 1:
            across_wait(q_ring, k - 1)
        if k == 1:
            across_in(wqs, dqs, dqr, z, 0).wait_recv()
            normalize()
        if k == 5:
            first_arrivals()
        if k == 8:
            relay()
        if k == 11:
            last_arrivals()
        for i, init in block_after.get(k, []):
            block(i, init)

    block(3)
    block(-3)
    across_wait(q_ring, half)
    block(4)
    loads[6].wait()
    loads[7].wait()
    attend(0)
    attend(1)

    @pl.loop(EARLY + 1, half - 1)
    def _(i):
        ring_step(w_ring, i)
        reduce_chunks(reached(i - 1), reached(i))

    for i in (half - 1, half):
        ring_step(w_ring, i)
        reduce_chunks(reached(i - 1), reached(i))
    at = reached(half)

    @pl.loop(at[0], nz)
    def _(q):
        stage_a(q)

    ring_drain(q_ring)
    ring_drain(w_ring)

    reduce_chunks((nz,) + at[1:], (nz,) * 4)

    whole = fin[...].reshape(width, rows)
    square = jnp.sum(whole * whole, axis=0, keepdims=True)
    tot2[t] = jnp.broadcast_to(square, (8, rows))
    for copy in share(tot2, usend, urecv):
        copy.start()
    res[...] = whole * pgain[:, 0:1]

    for copy in share(tot, tsend, trecv):
        copy.wait_send()
    remote(stage, nb.at[t], n1s.at[0], n1r.at[c], (g0 + 1 - y, z, 2 * x + y)).wait_send()

    @pl.when(c != y)
    def _():
        remote(stage, nb.at[t], n1s.at[1], n1r.at[c], peer).wait_send()

    for i in range(6):
        round_x(0, xp, i).wait_send()

    share_wait(tot2, usend, urecv)
    res[...] = tok[...].astype(F32) + res[...] * total_scale(tot2)
    out = local(res, out_ref, 9)
    out.start()

    @pl.loop(0, nz)
    def _(q):
        s, o, ox, oc = chunk_of(q)
        dx = lax.rem(x - ox + nx, nx)

        @pl.when((y != c) | (oc != c))
        def _():
            to_peer(s, 1 - c).wait_send()

        @pl.when((oc == c) & (dx == 2))
        def _():
            to_side(s, 0).wait_send()
            to_side(s, 1).wait_send()

        @pl.when((oc == c) & ((dx == 1) | (dx == 3)))
        def _():
            to_owner(s, dx // 2, xp).wait_send()

    for copy in share(tot2, usend, urecv):
        copy.wait_send()
    out.wait()


def rope_tables(length):
    half = HEAD_DIM // 2
    freq = np.float32(ROPE_BASE) ** (-(np.arange(half, dtype=np.float32) * np.float32(2.0) / np.float32(HEAD_DIM)))
    angle = np.arange(length, dtype=np.float32)[:, None] * freq.astype(np.float32)[None, :]
    cosine, sine = np.cos(angle), np.sin(angle)
    return (
        np.concatenate([cosine, cosine], axis=1).astype(np.float32),
        np.concatenate([-sine, sine], axis=1).astype(np.float32),
    )


def on_device(nz, nt, tokens, norm_gain, w_query, w_key, w_value, w_out, post_gain):
    rows, width = tokens.shape
    depth = w_query.shape[0]
    cosine, sine = rope_tables(rows)
    q_cols = w_query.shape[1] // 2
    qkv = q_cols + w_key.shape[1] // 2 + w_value.shape[1] // 2
    dma = pltpu.SemaphoreType.DMA
    half = nz // 2
    vm = pltpu.VMEM
    hbm = pl.BlockSpec(memory_space=pl.ANY)
    out = pl.pallas_call(
        functools.partial(kernel, nz, nt),
        out_shape=jax.ShapeDtypeStruct((width, rows), F32),
        in_specs=[hbm] * 9,
        out_specs=hbm,
        scratch_shapes=[
            vm((width, rows), BF16),
            vm((width,), BF16),
            vm((width,), BF16),
            vm((width, 128), F32),
            vm((rows, HEAD_DIM), F32),
            vm((rows, HEAD_DIM), F32),
            vm((2, nz, depth, qkv), BF16),
            vm((2, nz, depth, q_cols), BF16),
            vm((rows, width), BF16),
            vm((nt, rows, width), BF16),
            vm((2, rows, qkv), F32),
            vm((2, rows, q_cols), BF16),
            vm((2, nz, depth, rows), BF16),
            vm((nz, depth, rows), BF16),
            vm((nz, depth, rows), BF16),
            vm((nz, depth, 128), BF16),
            vm((2, nz, depth, rows), BF16),
            vm((nz // nt, depth, rows), F32),
            vm((width, rows), F32),
            vm((nt, 8, rows), F32),
            vm((nt, 8, rows), F32),
            dma((10,)),
            dma((2, SLOTS, PIECES)),
            dma((2, half, PIECES)),
            dma((2, SLOTS, PIECES)),
            dma((2, half, PIECES)),
            dma((2, SLOTS)),
            dma((nz,)),
            dma((2, SLOTS)),
            dma((nz,)),
            dma((nt,)),
            dma((nt,)),
            dma((nt,)),
            dma((nt,)),
            dma((2,)),
            dma((2,)),
            dma((6,)),
            dma((nt,)),
            dma((nz,)),
            dma((nz // 2,)),
            dma((nz // 2,)),
            dma((2, nz // nt)),
            dma((2, nz // nt)),
            dma((2, nz // nt)),
            dma((2, nz // nt)),
        ],
        compiler_params=pltpu.CompilerParams(
            collective_id=0, has_side_effects=True, vmem_limit_bytes=60 * 1024 * 1024
        ),
        name="attention_block",
    )(
        tokens.T,
        norm_gain,
        w_query,
        w_key,
        w_value,
        w_out.T,
        post_gain,
        jnp.asarray(cosine),
        jnp.asarray(sine),
    )
    return out.T


def solution(mesh):
    nz, nt = mesh.shape["fsdp"], mesh.shape["tensor"]
    placed = (
        P(("groups", "fsdp"), "tensor"),
        P("tensor"),
        P("fsdp", "tensor"),
        P("fsdp", "tensor"),
        P("fsdp", "tensor"),
        P("tensor", "fsdp"),
        P("tensor"),
    )
    return jax.shard_map(
        functools.partial(on_device, nz, nt),
        mesh=mesh,
        in_specs=placed,
        out_specs=P(("groups", "fsdp"), "tensor"),
        check_vma=False,
    )
```

```python
import functools

import jax
import jax.numpy as jnp
import numpy as np
from jax import lax
from jax.experimental import pallas as pl
from jax.experimental.pallas import tpu as pltpu
from jax.sharding import PartitionSpec as P

HEAD_DIM = 128
EPS = 1e-06
SOFT_CAP = 50.0
ATTN_SCALE = 144.0 ** (-0.5)
ROPE_BASE = 10000.0
MESH = pl.DeviceIdType.MESH
F32 = jnp.float32
BF16 = jnp.bfloat16

PIECES = 3
EARLY = 11
SLOTS = 4


def nt_dot(a, b):
    return lax.dot_general(a, b, (((1,), (1,)), ((), ())), preferred_element_type=F32)


def kernel(
    nz,
    nt,
    tokens_ref,
    gain_ref,
    wq_ref,
    wk_ref,
    wv_ref,
    wo_ref,
    post_ref,
    cos_ref,
    sin_ref,
    out_ref,
    tok,
    gain,
    post,
    pgain,
    cosine,
    sine,
    wqs,
    wos,
    stage,
    nb,
    acc,
    attn,
    pd,
    ybuf,
    sbuf,
    hbuf,
    abuf,
    xbuf,
    fin,
    res,
    tot,
    tot2,
    lsem,
    zqs,
    zqr,
    zws,
    zwr,
    dqs,
    dqr,
    dws,
    dwr,
    tsend,
    trecv,
    usend,
    urecv,
    n1s,
    n1r,
    n2s,
    n2r,
    psend,
    yrecv,
    drecv,
    hsend,
    hrecv,
    arecv,
    xsend,
    xrecv,
):
    g = lax.axis_index("groups")
    z = lax.axis_index("fsdp")
    t = lax.axis_index("tensor")
    y = lax.rem(g, 2)
    g0 = g - y
    x = t // 2
    c = lax.rem(t, 2)
    nx = nt // 2
    per_t = nz // nt
    half = nz // 2
    width, rows = tok.shape
    d_model = width * nt
    chunk = wqs.shape[2]
    piece = chunk // PIECES
    zn = (lax.rem(z + 1, nz), lax.rem(z + nz - 1, nz))
    xp, xm = lax.rem(x + 1, nx), lax.rem(x + nx - 1, nx)
    peer = (g, z, 2 * x + 1 - c)
    q_last = (half, half - 1)
    w_last = (half - 1, half)

    def local(src, dst, i):
        return pltpu.make_async_copy(src, dst, lsem.at[i])

    def remote(src, dst, ss, rs, dev):
        return pltpu.make_async_remote_copy(
            src_ref=src, dst_ref=dst, send_sem=ss, recv_sem=rs, device_id=dev, device_id_type=MESH
        )

    yq = pl.multiple_of(y * 256, 128)
    yk = pl.multiple_of(y * 128, 128)
    loads = [
        local(wq_ref.at[:, pl.ds(yq, 256)], wqs.at[c, z, :, pl.ds(0, 256)], 0),
        local(wk_ref.at[:, pl.ds(yk, 128)], wqs.at[c, z, :, pl.ds(256, 128)], 1),
        local(wv_ref.at[:, pl.ds(yk, 128)], wqs.at[c, z, :, pl.ds(384, 128)], 2),
        local(tokens_ref, tok, 3),
        local(gain_ref, gain, 4),
        local(wo_ref.at[:, pl.ds(yq, 256)], wos.at[c, z], 5),
        local(cos_ref, cosine, 6),
        local(sin_ref, sine, 7),
        local(post_ref, post, 8),
    ]
    for load in loads:
        load.start()

    barrier = pltpu.get_barrier_semaphore()
    partners = [(g, zn[0], t), (g, zn[1], t)]
    partners += [(g, z, lax.rem(t + i, nt)) for i in range(1, nt)]
    partners += [(g0 + 1 - y, z, 2 * x), (g0 + 1 - y, z, 2 * x + 1)]
    for dev in partners:
        pl.semaphore_signal(barrier, inc=1, device_id=dev, device_id_type=MESH)
    pl.semaphore_wait(barrier, len(partners))

    def source(d, k):
        return lax.rem(z - k + nz, nz) if d == 0 else lax.rem(z + k, nz)

    def order(d, k, last):
        if isinstance(k, int) and k == 0:
            return 0
        return 2 * k - 1 if d == 0 or (isinstance(k, int) and k == half) else 2 * k

    def ring_copy(buf, ss, rs, d, k, sem_k, p):
        ref = buf.at[c, source(d, k), pl.ds(p * piece, piece)]
        return remote(ref, ref, ss.at[d, 0, p], rs.at[d, sem_k, p], (g, zn[d], t))

    def across_in(buf, ss, rs, s, i):
        ref = buf.at[1 - c, s]
        return remote(ref, ref, ss.at[0, 0], rs.at[i], peer)

    q_ring = (wqs, zqs, zqr, dqs, dqr, q_last)
    w_ring = (wos, zws, zwr, dws, dwr, w_last)

    def slot(k):
        return k % SLOTS if isinstance(k, int) else lax.rem(k, SLOTS)

    def ring_send(ring, d, k, p):
        buf, ss, rs, ds, dr, last = ring
        ref = buf.at[c, source(d, k), pl.ds(p * piece, piece)]
        return remote(ref, ref, ss.at[d, slot(k), p], rs.at[d, k, p], (g, zn[d], t))

    def across_send(ring, d, k):
        buf, ss, rs, ds, dr, last = ring
        ref = buf.at[c, source(d, k)]
        return remote(ref, ref, ds.at[d, slot(k)], dr.at[order(d, k, last)], peer)

    def guarded(k, fn):
        if isinstance(k, int):
            if k >= SLOTS:
                fn()
        else:
            pl.when(k >= SLOTS)(fn)

    def ring_start(ring):
        for p in range(PIECES):
            for d in range(2):
                ring_send(ring, d, 0, p).start()
        across_send(ring, 0, 0).start()

    def ring_step(ring, k):
        buf, ss, rs, ds, dr, last = ring
        dirs = [d for d in range(2) if not isinstance(k, int) or k <= last[d]]
        for p in range(PIECES):
            for d in dirs:
                ring_copy(buf, ss, rs, d, k, k - 1, p).wait_recv()
                if not isinstance(k, int) or k < last[d]:
                    guarded(k, lambda: ring_send(ring, d, k, p).wait_send())
                    ring_send(ring, d, k, p).start()
        for d in dirs:
            if d == 0:
                guarded(k, lambda: across_send(ring, d, k).wait_send())
            elif isinstance(k, int):
                if k > SLOTS:
                    across_send(ring, d, k).wait_send()
            else:
                pl.when(k > SLOTS)(lambda: across_send(ring, d, k).wait_send())
            across_send(ring, d, k).start()

    def ring_drain(ring):
        buf, ss, rs, ds, dr, last = ring
        for d in range(2):
            for k in range(last[d] - SLOTS, last[d]):
                for p in range(PIECES):
                    ring_send(ring, d, k, p).wait_send()
            for k in range(last[d] - SLOTS + 1, last[d] + 1):
                across_send(ring, d, k).wait_send()

    def across_wait(ring, k):
        buf, ss, rs, ds, dr, last = ring
        for d in range(2):
            if not isinstance(k, int) or k <= last[d]:
                across_in(buf, ds, dr, source(d, k), order(d, k, last)).wait_recv()

    for i in (0, 1, 2):
        loads[i].wait()
    ring_start(q_ring)

    def share(buf, ss, rs):
        return [
            remote(buf.at[t], buf.at[t], ss.at[i], rs.at[t], (g, z, lax.rem(t + i, nt)))
            for i in range(1, nt)
        ]

    def share_wait(buf, ss, rs):
        for i in range(1, nt):
            o = lax.rem(t + nt - i, nt)
            remote(buf.at[o], buf.at[o], ss.at[i], rs.at[o], peer).wait_recv()

    def total_scale(buf):
        total = buf[0, 0:1]
        for i in range(1, nt):
            total = total + buf[i, 0:1]
        return lax.rsqrt(total / d_model + EPS)

    loads[3].wait()
    values = tok[...].astype(F32)
    tot[t] = jnp.broadcast_to(jnp.sum(values * values, axis=0, keepdims=True), (8, rows))
    for copy in share(tot, tsend, trecv):
        copy.start()

    loads[4].wait()
    loads[5].wait()
    loads[8].wait()
    pgain[...] = jnp.broadcast_to(post[...].astype(F32).reshape(1, width), (128, width)).T

    def first_hop(to_y):
        return remote(stage, nb.at[t], n1s.at[to_y], n1r.at[c], (g0 + to_y, z, 2 * x + y))

    def normalize():
        share_wait(tot, tsend, trecv)
        scaled = (tok[...].astype(F32) * total_scale(tot)).T
        stage[...] = (scaled * gain[...].astype(F32).reshape(1, width)).astype(BF16)
        first_hop_other = remote(
            stage, nb.at[t], n1s.at[0], n1r.at[c], (g0 + 1 - y, z, 2 * x + y)
        )
        first_hop_other.start()

        @pl.when(c == y)
        def _():
            nb[t] = stage[...]

        @pl.when(c != y)
        def _():
            remote(stage, nb.at[t], n1s.at[1], n1r.at[c], peer).start()

    def round_x(shard, to, i):
        return remote(
            nb.at[shard], nb.at[shard], n2s.at[i], n2r.at[shard], (g, z, 2 * to + c)
        )

    def first_arrivals():
        for i in range(2):
            shard = 2 * x + i

            @pl.when((y != c) | (c != i))
            def _():
                remote(nb.at[shard], nb.at[shard], n1s.at[0], n1r.at[i], peer).wait_recv()

            round_x(shard, xp, 2 * i).start()
            round_x(shard, xm, 2 * i + 1).start()

    def x_wait(shard):
        round_x(shard, xp, 0).wait_recv()

    def relay():
        x_wait(2 * xm)
        round_x(2 * xm, xp, 4).start()
        x_wait(2 * xp + 1)
        round_x(2 * xp + 1, xm, 5).start()

    def last_arrivals():
        opposite = lax.rem(x + 2, nx)
        x_wait(2 * xm + 1)
        x_wait(2 * xp)
        x_wait(2 * opposite)
        x_wait(2 * opposite + 1)

    first_block = z // per_t

    def block(i, init=False):
        o = lax.rem(first_block + i + nt, nt)
        feats = nb[o]
        for u in range(2):
            w = wqs[u, pl.ds(o * per_t, per_t)].reshape(width, wqs.shape[3])
            part = jnp.dot(feats, w, preferred_element_type=F32)
            acc[u] = part if init else acc[u] + part

    def rotary(values):
        return values * cosine[...] + pltpu.roll(values, HEAD_DIM // 2, 1) * sine[...]

    def attend(u):
        key = rotary(acc[u, :, 256:384]).astype(BF16)
        value = acc[u, :, 384:512].astype(BF16)
        spot_q = lax.broadcasted_iota(jnp.int32, (rows, rows), 0)
        spot_k = lax.broadcasted_iota(jnp.int32, (rows, rows), 1)
        for h in range(2):
            query = rotary(acc[u, :, h * 128 : (h + 1) * 128]).astype(BF16)
            scores = nt_dot(query, key) * ATTN_SCALE
            e = jnp.exp(SOFT_CAP * jnp.tanh(scores / SOFT_CAP))
            e = jnp.where(spot_k <= spot_q, e, 0.0)
            probs = (e / jnp.sum(e, axis=1, keepdims=True)).astype(BF16)
            out = jnp.dot(probs, value, preferred_element_type=F32)
            attn[u, :, h * 128 : (h + 1) * 128] = out.astype(BF16)

    def chunk_of(q):
        k = (q + 1) // 2
        s = lax.rem(jnp.where(lax.rem(q, 2) == 1, z - k + nz, z + k), nz)
        o = s // per_t
        return s, o, o // 2, lax.rem(o, 2)

    def owned(s):
        return s // (2 * per_t) * per_t + lax.rem(s, per_t)

    def to_peer(s, oc):
        return remote(
            pd.at[0, s], pd.at[1, s], psend.at[s], drecv.at[owned(s)], (g, z, 2 * x + oc)
        )

    def to_pair(s, oc):
        return remote(
            pd.at[0, s],
            ybuf.at[s],
            psend.at[s],
            yrecv.at[owned(s)],
            (g0 + 1 - y, z, 2 * x + oc),
        )

    def stage_a(q):
        s, o, ox, oc = chunk_of(q)
        across_in(wos, dws, dwr, s, q).wait_recv()
        part = nt_dot(wos[0, s], attn[0]) + nt_dot(wos[1, s], attn[1])
        pd[0, s] = part.astype(BF16)
        dx = lax.rem(x - ox + nx, nx)

        @pl.when((dx == 2) & (y == c))
        def _():
            to_side(s, 0, oc).start()
            to_side(s, 1, oc).start()

        @pl.when((dx == 2) & (y != c))
        def _():
            to_side_away(s, 0).start()
            to_side_away(s, 1).start()

        @pl.when((dx != 2) & (y == c) & (oc != c))
        def _():
            to_peer(s, oc).start()

        @pl.when((dx == 0) & (y != c))
        def _():
            to_pair(s, oc).start()

    away = jnp.where(y == c, 0, 1)

    def pair_sum(s):
        to_pair(s, c).wait_recv()

        @pl.when(y != c)
        def _():
            to_peer(s, c).wait_recv()

        return pd[away, s].astype(F32) + ybuf[s].astype(F32)

    def to_side(s, i, oc):
        return remote(
            pd.at[0, s, :, pl.ds(128 * i, 128)],
            hbuf.at[s],
            hsend.at[i, lax.rem(s, 2 * per_t)],
            hrecv.at[i, lax.rem(s, per_t)],
            (g, z, 2 * (xp, xm)[i] + oc),
        )

    def to_side_away(s, i):
        return remote(
            pd.at[0, s, :, pl.ds(128 * i, 128)],
            abuf.at[s],
            hsend.at[i, lax.rem(s, 2 * per_t)],
            arecv.at[i, lax.rem(s, 2 * per_t)],
            (g, z, 2 * (xp, xm)[i] + c),
        )

    def stage_b(q):
        s, o, ox, oc = chunk_of(q)
        dx = lax.rem(x - ox + nx, nx)
        for i in range(2):

            @pl.when((y != c) & (dx == 3 - 2 * i))
            def _():
                to_side_away(s, i).wait_recv()
                span = slice(128 * i, 128 * i + 128)
                pd[0, s, :, span] = (
                    pd[0, s, :, span].astype(F32) + abuf[s].astype(F32)
                ).astype(BF16)
                to_pair(s, oc).start()

    def to_owner(s, side, ox):
        return remote(
            sbuf.at[s],
            xbuf.at[side, s],
            xsend.at[side, lax.rem(s, per_t)],
            xrecv.at[side, lax.rem(s, per_t)],
            (g, z, 2 * ox + c),
        )

    def stage_c(q):
        s, o, ox, oc = chunk_of(q)
        dx = lax.rem(x - ox + nx, nx)

        @pl.when((oc == c) & ((dx == 1) | (dx == 3)))
        def _():
            total = pair_sum(s)
            @pl.when(dx == 3)
            def _():
                to_side(s, 0, c).wait_recv()

            @pl.when(dx == 1)
            def _():
                to_side(s, 1, c).wait_recv()

            extra = hbuf[s].astype(F32)
            sbuf[s, :, 0:128] = (total[:, 0:128] + jnp.where(dx == 3, extra, 0.0)).astype(BF16)
            sbuf[s, :, 128:256] = (total[:, 128:256] + jnp.where(dx == 1, extra, 0.0)).astype(BF16)
            to_owner(s, dx // 2, ox).start()

    def stage_d(q):
        s, o, ox, oc = chunk_of(q)

        @pl.when(o == t)
        def _():
            total = pair_sum(s)
            for side in range(2):
                to_owner(s, side, x).wait_recv()
                total = total + xbuf[side, s].astype(F32)
            fin[lax.rem(s, per_t)] = total

    def clipped(value, low, high):
        if isinstance(value, int):
            return max(min(value, high), low)
        return jnp.maximum(jnp.minimum(value, high), low)

    def reached(i):
        a = clipped(8 * (i - EARLY), 0, 2 * i - 1)
        before = clipped(8 * (i - 1 - EARLY), 0, 2 * i - 3)
        b = clipped(4 * (i - 1 - EARLY), 0, before)
        return a, b, clipped(5 * (i - EARLY) - 16, 0, b), clipped(5 * (i - EARLY) - 22, 0, b)

    def reduce_chunks(low, high):
        for fn, lo, hi in zip((stage_a, stage_b, stage_c, stage_d), low, high):

            @pl.loop(lo, hi)
            def _(q):
                fn(q)

    w_start = half - EARLY
    block_after = {
        half - 4: [(0, True), (1, False)],
        half - 3: [(-1, False), (2, False)],
        half - 2: [(-2, False)],
    }
    for k in range(1, half + 1):
        ring_step(q_ring, k)
        if k == w_start:
            ring_start(w_ring)
        if k > w_start:
            ring_step(w_ring, k - w_start)
        if k > 1:
            across_wait(q_ring, k - 1)
        if k == 1:
            across_in(wqs, dqs, dqr, z, 0).wait_recv()
            normalize()
        if k == 5:
            first_arrivals()
        if k == 8:
            relay()
        if k == 11:
            last_arrivals()
        for i, init in block_after.get(k, []):
            block(i, init)

    block(3)
    block(-3)
    across_wait(q_ring, half)
    block(4)
    loads[6].wait()
    loads[7].wait()
    attend(0)
    attend(1)

    @pl.loop(EARLY + 1, half - 1)
    def _(i):
        ring_step(w_ring, i)
        reduce_chunks(reached(i - 1), reached(i))

    for i in (half - 1, half):
        ring_step(w_ring, i)
        reduce_chunks(reached(i - 1), reached(i))
    at = reached(half)

    @pl.loop(at[0], nz)
    def _(q):
        stage_a(q)

    ring_drain(q_ring)
    ring_drain(w_ring)

    reduce_chunks((nz,) + at[1:], (nz,) * 4)

    whole = fin[...].reshape(width, rows)
    square = jnp.sum(whole * whole, axis=0, keepdims=True)
    tot2[t] = jnp.broadcast_to(square, (8, rows))
    for copy in share(tot2, usend, urecv):
        copy.start()
    res[...] = whole * pgain[:, 0:1]

    for copy in share(tot, tsend, trecv):
        copy.wait_send()
    remote(stage, nb.at[t], n1s.at[0], n1r.at[c], (g0 + 1 - y, z, 2 * x + y)).wait_send()

    @pl.when(c != y)
    def _():
        remote(stage, nb.at[t], n1s.at[1], n1r.at[c], peer).wait_send()

    for i in range(6):
        round_x(0, xp, i).wait_send()

    share_wait(tot2, usend, urecv)
    res[...] = tok[...].astype(F32) + res[...] * total_scale(tot2)
    out = local(res, out_ref, 9)
    out.start()

    @pl.loop(0, nz)
    def _(q):
        s, o, ox, oc = chunk_of(q)
        dx = lax.rem(x - ox + nx, nx)

        @pl.when((dx != 2) & ((y != c) | (oc != c)))
        def _():
            to_peer(s, 1 - c).wait_send()

        @pl.when(dx == 2)
        def _():
            to_side(s, 0, c).wait_send()
            to_side(s, 1, c).wait_send()

        @pl.when((oc == c) & ((dx == 1) | (dx == 3)))
        def _():
            to_owner(s, dx // 2, xp).wait_send()

    for copy in share(tot2, usend, urecv):
        copy.wait_send()
    out.wait()


def rope_tables(length):
    half = HEAD_DIM // 2
    freq = np.float32(ROPE_BASE) ** (-(np.arange(half, dtype=np.float32) * np.float32(2.0) / np.float32(HEAD_DIM)))
    angle = np.arange(length, dtype=np.float32)[:, None] * freq.astype(np.float32)[None, :]
    cosine, sine = np.cos(angle), np.sin(angle)
    return (
        np.concatenate([cosine, cosine], axis=1).astype(np.float32),
        np.concatenate([-sine, sine], axis=1).astype(np.float32),
    )


def on_device(nz, nt, tokens, norm_gain, w_query, w_key, w_value, w_out, post_gain):
    rows, width = tokens.shape
    depth = w_query.shape[0]
    cosine, sine = rope_tables(rows)
    q_cols = w_query.shape[1] // 2
    qkv = q_cols + w_key.shape[1] // 2 + w_value.shape[1] // 2
    dma = pltpu.SemaphoreType.DMA
    half = nz // 2
    vm = pltpu.VMEM
    hbm = pl.BlockSpec(memory_space=pl.ANY)
    out = pl.pallas_call(
        functools.partial(kernel, nz, nt),
        out_shape=jax.ShapeDtypeStruct((width, rows), F32),
        in_specs=[hbm] * 9,
        out_specs=hbm,
        scratch_shapes=[
            vm((width, rows), BF16),
            vm((width,), BF16),
            vm((width,), BF16),
            vm((width, 128), F32),
            vm((rows, HEAD_DIM), F32),
            vm((rows, HEAD_DIM), F32),
            vm((2, nz, depth, qkv), BF16),
            vm((2, nz, depth, q_cols), BF16),
            vm((rows, width), BF16),
            vm((nt, rows, width), BF16),
            vm((2, rows, qkv), F32),
            vm((2, rows, q_cols), BF16),
            vm((2, nz, depth, rows), BF16),
            vm((nz, depth, rows), BF16),
            vm((nz, depth, rows), BF16),
            vm((nz, depth, 128), BF16),
            vm((nz, depth, 128), BF16),
            vm((2, nz, depth, rows), BF16),
            vm((nz // nt, depth, rows), F32),
            vm((width, rows), F32),
            vm((nt, 8, rows), F32),
            vm((nt, 8, rows), F32),
            dma((10,)),
            dma((2, SLOTS, PIECES)),
            dma((2, half, PIECES)),
            dma((2, SLOTS, PIECES)),
            dma((2, half, PIECES)),
            dma((2, SLOTS)),
            dma((nz,)),
            dma((2, SLOTS)),
            dma((nz,)),
            dma((nt,)),
            dma((nt,)),
            dma((nt,)),
            dma((nt,)),
            dma((2,)),
            dma((2,)),
            dma((6,)),
            dma((nt,)),
            dma((nz,)),
            dma((nz // 2,)),
            dma((nz // 2,)),
            dma((2, 2 * nz // nt)),
            dma((2, nz // nt)),
            dma((2, 2 * nz // nt)),
            dma((2, nz // nt)),
            dma((2, nz // nt)),
        ],
        compiler_params=pltpu.CompilerParams(
            collective_id=0, has_side_effects=True, vmem_limit_bytes=60 * 1024 * 1024
        ),
        name="attention_block",
    )(
        tokens.T,
        norm_gain,
        w_query,
        w_key,
        w_value,
        w_out.T,
        post_gain,
        jnp.asarray(cosine),
        jnp.asarray(sine),
    )
    return out.T


def solution(mesh):
    nz, nt = mesh.shape["fsdp"], mesh.shape["tensor"]
    placed = (
        P(("groups", "fsdp"), "tensor"),
        P("tensor"),
        P("fsdp", "tensor"),
        P("fsdp", "tensor"),
        P("fsdp", "tensor"),
        P("tensor", "fsdp"),
        P("tensor"),
    )
    return jax.shard_map(
        functools.partial(on_device, nz, nt),
        mesh=mesh,
        in_specs=placed,
        out_specs=P(("groups", "fsdp"), "tensor"),
        check_vma=False,
    )
```
